32 devices in a mesh: edp: 8 (over z, core), ep: 4 (over y, x).
Axes of the slice: x: 2, y: 2, z: 4, core: 2. Of those that a mesh axis runs over, the one named last changes fastest.
Arguments:
- route_ids: int32 [4096, 8], P(('edp', 'ep')), may hold values from 0 to 127, all different within a row; in each aligned block of 128 rows (0 to 127, 128 to 255, ...) at most 16 rows name the same one
- route_weights: float32 [4096, 8], P(('edp', 'ep')), may hold values from 0.02 to 0.5
- hidden: bfloat16 [8, 4, 4, 16, 384], P('edp', 'ep'), may hold values from -6 to 6
- down_weight: bfloat16 [4, 384, 2048], P('ep', 'edp'), may hold values from -0.3125 to 0.3125
- cotangent: bfloat16 [4096, 2048], P(('edp', 'ep')), may hold values from -6 to 6
Outputs:
- layer_out: bfloat16 [4096, 2048], P(('edp', 'ep'))
- route_grad: float32 [4096, 8], P(('edp', 'ep'))
- hidden_grad: bfloat16 [8, 4, 4, 16, 384], P('edp', 'ep')
- weight_grad: float32 [4, 384, 2048], P('ep', 'edp')
The draws below stay inside these ranges and needn't reach their ends.
Inputs may be any that keep to these rules, and one draw needn't show every extreme that they name: `route_ids`: each row names 8 different experts; in the 128 rows of one device no expert is named by more than 16 rows.
All inputs are finite; a program needn't handle non-finite values.
Results may differ from the reference program's by a relative error of at most 0.0049.
Values may be sent and summed in bfloat16 or wider, within the bound.
No kernel may reach another device: no remote copies, remote signals or barrier semaphores. Data moves between devices by JAX's collectives and lax.ppermute only.
A program may use at most 64 MiB of HBM per device.

```python
import math
import jax
import jax.numpy as jnp
import numpy as np
from jax import lax

D = 2048
EXPERTS = 128
TOP = 8
FF = 384
TOK_DEV = 128
CAP = 16
WIN = 4
TOKENS = 4096
N_EDP = 8
N_EP = 4


def spiked(values, stream_key, source, target, shards_of, factor):
    owner, partner = [(jnp.arange(values.shape[position]) // (values.shape[position] // shards_of)).reshape([-1 if axis == position else 1 for axis in range(values.ndim)]) for position in (source, target)]
    chosen = jax.random.permutation(stream_key, shards_of)[partner]
    strong = (owner == chosen) | (owner == (partner + shards_of // 2) % shards_of)
    return jnp.where(strong, factor * values, values)


def levels(key, shape, split, smallest, largest):
    def one(dim, blocks):
        steps = jax.random.uniform(jax.random.fold_in(jax.random.fold_in(key, 6), dim), (blocks,), jnp.float32, smallest / len(split), largest / len(split))
        return jnp.repeat(jnp.exp(steps), shape[dim] // blocks).reshape((-1,) + (1,) * (len(shape) - dim - 1))

    factor_of = one(*split[0])
    for cut in split[1:]:
        factor_of = factor_of * one(*cut)
    return factor_of


def shared_out(key, own, number, rows, amount, top, bound, lean):
    order = jax.random.permutation(key, amount)
    packed, common = shares(amount, rows * top, bound, lean, True), shares(amount, rows * top, bound, lean, False)
    places = jnp.arange(amount)

    def named(sizes, rotation):
        used = int((sizes > 0).sum())
        fixed = max(1, used // 4)
        passed = fixed + (places - fixed + rotation * (used - fixed)) % max(1, amount - fixed)
        return jnp.zeros((amount,), jnp.int32).at[order[jnp.where(places < fixed, places, passed)]].set(jnp.asarray(sizes, jnp.int32))

    sizes = jnp.where(number % 4 == 0, named(packed, number // 4), named(common, number - number // 4 - 1))
    mixed = jax.random.permutation(jax.random.fold_in(own, 3), amount)
    giver, receiver = mixed[0:amount // 2 * 2:2], mixed[1:amount // 2 * 2:2]
    room = jnp.minimum(sizes[giver] - 1, bound - sizes[receiver]) // 2
    room = jnp.where((giver == order[0]) | (receiver == order[0]) | (sizes[receiver] == 0), 0, jnp.maximum(room, 0))
    passed = jax.random.randint(jax.random.fold_in(own, 4), (amount // 2,), 0, 1 << 20) % (room + 1)
    sizes = sizes.at[giver].add(-passed).at[receiver].add(passed)
    items = jnp.searchsorted(jnp.cumsum(sizes), jnp.arange(rows * top), side="right").astype(jnp.int32)
    table = items.reshape(top, rows).T
    table = table[jax.random.permutation(jax.random.fold_in(own, 1), rows)]
    rotation = jax.random.randint(jax.random.fold_in(own, 2), (rows, 1), 0, top)
    return jnp.take_along_axis(table, (jnp.arange(top)[None, :] + rotation) % top, axis=1)


def shares(amount, total, bound, lean, full):
    weights = [(1 << 20) // math.isqrt(standing ** lean) + 1 for standing in range(1, amount + 1)]
    largest = bound if full else min(bound, max(-(-total // amount), total * weights[0] // sum(weights)))
    least = 1 if total - largest >= amount - 1 else 0
    counts, surplus = [largest] + [least] * (amount - 1), total - largest - least * (amount - 1)
    while surplus > 0:
        candidates = [i for i in range(1, amount) if counts[i] < largest] or [i for i in range(1, amount) if counts[i] < bound]
        mass, budget = sum([weights[i] for i in candidates]), surplus
        for i in candidates:
            addition = min(bound - counts[i], max(1, budget * weights[i] // mass), surplus)
            counts[i] = counts[i] + addition
            surplus = surplus - addition
    return np.array(counts)


def normal_values(rng, extent, deviation, bound, pieces=(), kind=jnp.bfloat16):
    level = levels(rng, extent, pieces, -0.22, 0.18) if pieces else 1.0
    array = jax.random.normal(rng, extent, jnp.float32) * deviation * level
    return jnp.minimum(jnp.maximum(array, -bound), bound).astype(kind)


def heavy_noise(key, extent, spread, reach, pieces, heavy, kind=jnp.bfloat16):
    result = spread * jax.random.normal(key, extent, jnp.float32)
    if pieces:
        result = result * levels(key, extent, pieces, -0.22, 0.18)
    return jnp.clip(spiked(result, jax.random.fold_in(key, 3), *heavy), -reach, reach).astype(kind)


def setup_inputs(seed: int = 0) -> dict:
    streams_of = jax.random.split(jax.random.key(seed), 6)
    route_ids_keys = jax.random.split(jax.random.fold_in(streams_of[0], 1), TOKENS // TOK_DEV)
    route_ids_turns = jax.random.permutation(jax.random.fold_in(streams_of[0], 3), TOKENS // TOK_DEV)
    route_ids = jax.vmap(lambda own, number: shared_out(jax.random.fold_in(streams_of[0], 2), own, number, TOK_DEV, EXPERTS, TOP, CAP, 2))(route_ids_keys, route_ids_turns).reshape((TOKENS, TOP))
    route_weights = jnp.clip(jnp.exp(math.log(0.5) - 3.218876 * jax.random.uniform(streams_of[1], (TOKENS, TOP), jnp.float32) ** levels(streams_of[1], (TOKENS, TOP), ((0, 32),), -0.2, 0.2)), 0.02, 0.5)
    hidden = heavy_noise(streams_of[2], (N_EDP, WIN, N_EP, CAP, FF), 1.0, 6.0, ((0, 8), (1, 4)), (0, 4, 8, 2.0))
    down_weight = normal_values(streams_of[3], (WIN, FF, D), FF ** -0.5, 0.3125, ((0, 4), (1, 8)))
    cotangent = normal_values(streams_of[4], (TOKENS, D), 1.0, 6.0, ((0, 32),))
    return dict(route_ids=route_ids, route_weights=route_weights, hidden=hidden, down_weight=down_weight, cotangent=cotangent)


def reference(route_ids, route_weights, hidden, down_weight, cotangent):
    experts_here = N_EP
    capacity = CAP
    groups = N_EDP
    ids_grouped = route_ids.reshape(groups, N_EP, TOK_DEV, TOP)
    probs_grouped = route_weights.reshape(groups, N_EP, TOK_DEV, TOP)
    cot_grouped = cotangent.reshape(groups, N_EP, TOK_DEV, D)
    weight_f32 = down_weight.astype(jnp.float32)
    labels = jnp.arange(experts_here, dtype=jnp.int32)
    source = jnp.arange(N_EP, dtype=jnp.int32)[:, None, None]

    def one_group(summed, inputs):
        ids_group, prob_group, cot_group, hid_group = inputs
        onehot = jnp.sum((ids_group[..., None] == labels).astype(jnp.int32), axis=2).astype(jnp.int32)
        preceding = (jnp.cumsum(onehot, axis=1) - onehot).astype(jnp.int32)
        flight = ids_group < experts_here
        expert = jnp.where(flight, ids_group, 0).astype(jnp.int32)
        slot_rank = jnp.take_along_axis(preceding, expert, axis=2).astype(jnp.int32)
        slot_index = ((expert * N_EP + source) * capacity + slot_rank).astype(jnp.int32)
        hid_f = hid_group.astype(jnp.float32)
        expert_out = jnp.einsum("escf,efd->escd", hid_f, weight_f32, precision=lax.Precision.HIGHEST).astype(jnp.bfloat16)
        lookup = expert_out.reshape(-1, D)
        picked = jnp.take(lookup, slot_index, axis=0).astype(jnp.float32)
        mixing = jnp.where(flight, prob_group, jnp.float32(0.0))
        combined = jnp.sum(mixing[..., None] * picked, axis=2).astype(jnp.bfloat16)
        cot_f = cot_group.astype(jnp.float32)
        route_grad = jnp.where(flight, jnp.sum(cot_f[:, :, None, :] * picked, axis=3), jnp.float32(0.0))
        weighted = mixing[..., None] * cot_f[:, :, None, :]
        slot_grad = jnp.zeros((experts_here * N_EP * capacity, D), jnp.float32)
        slot_grad = slot_grad.at[slot_index.reshape(-1)].add(weighted.reshape(-1, D))
        slot_grad = slot_grad.astype(jnp.bfloat16).reshape(experts_here, N_EP, capacity, D)
        grad_f = slot_grad.astype(jnp.float32)
        hidden_grad = jnp.einsum("escd,efd->escf", grad_f, weight_f32, precision=lax.Precision.HIGHEST).astype(jnp.bfloat16)
        summed = summed + jnp.einsum("escf,escd->efd", hid_f, grad_f, precision=lax.Precision.HIGHEST)
        return summed, (combined, route_grad, hidden_grad)

    start = jnp.zeros((experts_here, FF, D), jnp.float32)
    weight_grad, stacked = lax.scan(one_group, start, (ids_grouped, probs_grouped, cot_grouped, hidden))
    combined, route_grad, hidden_grad = stacked
    return (combined.reshape(TOKENS, D), route_grad.reshape(TOKENS, TOP), hidden_grad, weight_grad)
```

```python
import functools

import jax
import jax.numpy as jnp
from jax import lax
from jax.experimental import pallas as pl
from jax.experimental.pallas import tpu as pltpu
from jax.sharding import Mesh
from jax.sharding import PartitionSpec as P

BF16 = jnp.bfloat16
F32 = jnp.float32
NN = (((1,), (0,)), ((), ()))
NT = (((1,), (1,)), ((), ()))
TN = (((0,), (0,)), ((), ()))


def dot(a, b, dims):
    return lax.dot_general(a, b, dims, preferred_element_type=F32)


def call(body, outs, scratch=(), flops=0, name=None):
    size = sum(o.size * o.dtype.itemsize for o in jax.tree.leaves(outs))
    return pl.pallas_call(
        body,
        out_shape=outs,
        scratch_shapes=scratch,
        name=name,
        cost_estimate=pl.CostEstimate(flops=flops, bytes_accessed=2 * size, transcendentals=0),
    )


def sds(shape, dtype):
    return jax.ShapeDtypeStruct(shape, dtype)


def aligned(index, size, unit):
    return pl.ds(pl.multiple_of(index * size, unit), size)


def halves_body(w_ref, same_ref, cross_ref):
    h = lax.axis_index("h")
    half = same_ref.shape[1]
    same_ref[...] = w_ref[:, aligned(h, half, 128)]
    cross_ref[...] = w_ref[:, aligned(1 - h, half, 128)]


def route_body(experts, capacity, ids_ref, weight_ref, cot_ref, sent_ref, table_ref, index_ref):
    ids = ids_ref[...]
    weights = weight_ref[...]
    tokens = ids.shape[1]
    half = sent_ref.shape[2]
    row = lax.broadcasted_iota(jnp.int32, (tokens, tokens), 0)
    col = lax.broadcasted_iota(jnp.int32, (tokens, tokens), 1)
    earlier = jnp.where(row < col, 1.0, 0.0).astype(BF16)
    named = [jnp.sum(jnp.where(ids == e, 1.0, 0.0), axis=0, keepdims=True) for e in range(experts)]
    mixing = [jnp.sum(jnp.where(ids == e, weights, 0.0), axis=0, keepdims=True) for e in range(experts)]
    preceding = dot(jnp.concatenate(named, axis=0).astype(BF16), earlier, NN)
    slot = lax.broadcasted_iota(jnp.int32, (capacity, tokens), 0).astype(F32)
    chosen, combine = [], []
    index = jnp.full(ids.shape, -1.0, F32)
    for e in range(experts):
        rank = preceding[e : e + 1]
        match = jnp.where(rank == slot, 1.0, 0.0) * named[e]
        chosen.append(match)
        combine.append(match * mixing[e])
        index = jnp.where(ids == e, rank + float(e * capacity), index)
    index_ref[...] = index
    chosen = jnp.concatenate(chosen, axis=0)
    combine = jnp.concatenate(combine, axis=0)
    slots = chosen.shape[0]
    slot_weight = jnp.sum(combine, axis=1, keepdims=True)
    high = combine.astype(BF16)
    rest = combine - high.astype(F32)
    middle = rest.astype(BF16)
    table_ref[0:slots] = high
    table_ref[slots : 2 * slots] = middle
    table_ref[2 * slots : 3 * slots] = (rest - middle.astype(F32)).astype(BF16)
    gathered = dot(chosen.astype(BF16), cot_ref[...], NN)
    value = (gathered * slot_weight).astype(BF16)
    for g in range(2):
        for e in range(experts):
            sent_ref[g * experts + e] = value[e * capacity : (e + 1) * capacity, g * half : (g + 1) * half]


def expert_body(moves, groups, *refs):
    count = len(moves)
    blocks = refs[: 2 * count]
    own_ref, pair_ref, out_ref, full_ref, hid_ref, stage_ref = refs[2 * count :]
    q, h, c = lax.axis_index("q"), lax.axis_index("h"), lax.axis_index("c")
    rows = blocks[0].shape[0]
    slots = own_ref.shape[0]
    for i, (dq, dh) in enumerate(moves):
        source = (lax.rem(q + (groups - dq), groups) * 2 + lax.rem(h + dh, 2)) * 2
        stage_ref[aligned(source + c, rows, 8), :] = blocks[i][...].astype(stage_ref.dtype)
        stage_ref[aligned(source + 1 - c, rows, 8), :] = blocks[count + i][...].astype(stage_ref.dtype)
    hid_ref[aligned(h, slots, 16), :] = own_ref[...]
    hid_ref[aligned(1 - h, slots, 16), :] = pair_ref[...]
    full = stage_ref[...].astype(BF16)
    full_ref[...] = full
    out_ref[...] = dot(hid_ref[...], full, NN).astype(BF16).reshape(out_ref.shape)


def hidden_grad_body(grad_ref, full_ref, keep_ref, send_ref):
    h = lax.axis_index("h")
    n = grad_ref.shape[0] // 2
    flat = (n * grad_ref.shape[1], grad_ref.shape[2])
    full = full_ref[...]
    keep_ref[...] = dot(grad_ref[pl.ds(h * n, n)].reshape(flat), full, NT)
    send_ref[...] = dot(grad_ref[pl.ds((1 - h) * n, n)].reshape(flat), full, NT).astype(BF16)


def weight_grad_body(moves, groups, own_ref, h_ref, c_ref, hc_ref, grad_ref, partner_ref, *refs):
    count = len(moves)
    outs, (hid_ref, total_ref) = refs[:count], refs[count:]
    q, h, c = lax.axis_index("q"), lax.axis_index("h"), lax.axis_index("c")
    slots = own_ref.shape[0]
    rows = outs[0].shape[0]
    hid_ref[aligned(h, slots, 16), :] = own_ref[...]
    hid_ref[aligned(1 - h, slots, 16), :] = h_ref[...]
    hid_ref[aligned(2 + h, slots, 16), :] = c_ref[...]
    hid_ref[aligned(3 - h, slots, 16), :] = hc_ref[...]
    flat = (2 * slots, grad_ref.shape[2])
    grads = jnp.concatenate([grad_ref[...].reshape(flat), partner_ref[...].reshape(flat)], axis=0)
    total_ref[...] = dot(hid_ref[...], grads, TN)
    for (dq, dh), out in zip(moves, outs, strict=True):
        target = (lax.rem(q + dq, groups) * 2 + lax.rem(h + dh, 2)) * 2 + c
        out[...] = total_ref[aligned(target, rows, 8), :].astype(out.dtype)


def combine_body(arrived_ref, table_ref, index_ref, cot_ref, layer_ref, route_ref):
    n, capacity, half = arrived_ref.shape
    slots = n // 2 * capacity
    scores = None
    for g in range(2):
        rows = arrived_ref[g * (n // 2) : (g + 1) * (n // 2)].reshape(slots, half)
        mixed = dot(table_ref[...], jnp.concatenate([rows] * 3, axis=0), TN)
        layer_ref[:, g * half : (g + 1) * half] = mixed.astype(BF16)
        part = dot(rows, cot_ref[:, g * half : (g + 1) * half], NT)
        scores = part if scores is None else scores + part
    position = lax.broadcasted_iota(jnp.int32, scores.shape, 0).astype(F32)
    for k in range(index_ref.shape[0]):
        hit = position == index_ref[k : k + 1]
        route_ref[k : k + 1] = jnp.sum(jnp.where(hit, scores, 0.0), axis=0, keepdims=True)


def finish_body(moves, keep_ref, arrived_ref, *refs):
    count = len(moves)
    terms, (hidden_ref, weight_ref) = refs[:count], refs[count:]
    h = lax.axis_index("h")
    half = terms[0].shape[1]
    hidden_ref[...] = (keep_ref[...] + arrived_ref[...].astype(F32)).astype(BF16)
    for side in range(2):
        total = None
        for (_, dh), term in zip(moves, terms, strict=True):
            if dh == side:
                value = term[...].astype(F32)
                total = value if total is None else total + value
        weight_ref[:, aligned(h if side == 0 else 1 - h, half, 128)] = total


def local(route_ids, route_weights, hidden, down_weight, cotangent):
    groups = lax.axis_size("q")
    experts = lax.axis_size("ep")
    tokens, features = cotangent.shape
    capacity, width = hidden.shape[3], hidden.shape[4]
    rows = down_weight.shape[1]
    slots = experts * capacity
    half = features // 2
    moves = [(0, 0), (0, 1)] + [(dq, dh) for dq in range(1, groups) for dh in range(2)]
    chips = ("q", "h")
    swap = [(0, 1), (1, 0)]

    def move(x, step):
        dq, dh = step
        pairs = [(a * 2 + b, (a + dq) % groups * 2 + (b + dh) % 2) for a in range(groups) for b in range(2)]
        return lax.ppermute(x, chips, pairs)

    def swap_core(x):
        return lax.ppermute(x, "c", swap)

    shard = down_weight[0]
    piece = sds((rows, half), BF16)
    same, cross = call(halves_body, (piece, piece), name="halves")(shard)
    blocks = [same] + [move(cross if dh else same, (dq, dh)) for dq, dh in moves[1:]]
    blocks = blocks + [swap_core(b) for b in blocks]

    own = hidden.reshape(slots, width)
    pair = lax.ppermute(own, "h", swap)
    partner = swap_core(own)
    diagonal = lax.ppermute(own, ("h", "c"), [(i, 3 - i) for i in range(4)])

    parts = sds((2 * experts, capacity, half), BF16)
    sent, table, index = call(
        functools.partial(route_body, experts, capacity),
        (parts, sds((3 * slots, tokens), BF16), sds((route_ids.shape[1], tokens), F32)),
        flops=2 * slots * tokens * features,
        name="route",
    )(route_ids.T, route_weights.T, cotangent)
    grads = lax.all_to_all(sent, ("h", "ep"), split_axis=0, concat_axis=0, tiled=True)
    partner_grads = swap_core(grads)

    weight_out = call(
        functools.partial(weight_grad_body, moves, groups),
        tuple(sds((rows, half), BF16 if i else F32) for i in range(len(moves))),
        [pltpu.VMEM((4 * slots, width), BF16), pltpu.VMEM((width, half), F32)],
        flops=2 * 4 * slots * width * half,
        name="weight_grad",
    )(own, pair, partner, diagonal, grads, partner_grads)
    terms = [weight_out[0]] + [move(x, step) for x, step in zip(weight_out[1:], moves[1:], strict=True)]

    expert_out, full = call(
        functools.partial(expert_body, moves, groups),
        (parts, sds((width, half), BF16)),
        [pltpu.VMEM((2 * slots, width), BF16), pltpu.VMEM((width, half), BF16 if rows % 16 == 0 else F32)],
        flops=2 * 2 * slots * width * half,
        name="expert",
    )(*blocks, own, pair)
    arrived = lax.all_to_all(expert_out, ("h", "ep"), split_axis=0, concat_axis=0, tiled=True)

    keep, give = call(
        hidden_grad_body,
        (sds((slots, width), F32), sds((slots, width), BF16)),
        flops=2 * 2 * slots * width * half,
        name="hidden_grad",
    )(grads, full)
    taken = lax.ppermute(give, "h", swap)

    layer_out, route_grad = call(
        combine_body,
        (sds((tokens, features), BF16), sds((route_ids.shape[1], tokens), F32)),
        flops=2 * 4 * slots * tokens * features,
        name="combine",
    )(arrived, table, index, cotangent)

    hidden_grad, weight_grad = call(
        functools.partial(finish_body, moves),
        (sds((slots, width), BF16), sds((rows, features), F32)),
        flops=rows * features,
        name="finish",
    )(keep, taken, *terms)
    return layer_out, route_grad.T, hidden_grad.reshape(hidden.shape), weight_grad[None]


def solution(mesh):
    edp, ep = mesh.shape["edp"], mesh.shape["ep"]
    fine = Mesh(mesh.devices.reshape(edp // 4, 2, 2, ep), ("q", "h", "c", "ep"))
    group = ("q", "h", "c")
    tokens = P(group + ("ep",), None)
    slots = P(group, "ep", None, None, None)
    weights = P("ep", group, None)
    return jax.shard_map(
        local,
        mesh=fine,
        in_specs=(tokens, tokens, slots, weights, tokens),
        out_specs=(tokens, tokens, slots, weights),
        check_vma=False,
    )
```

```python
import functools

import jax
import jax.numpy as jnp
from jax import lax
from jax.experimental import pallas as pl
from jax.experimental.pallas import tpu as pltpu
from jax.sharding import Mesh
from jax.sharding import PartitionSpec as P


LOAD_LIMIT = 16 * 2**20
BF16 = jnp.bfloat16
F32 = jnp.float32
NN = (((1,), (0,)), ((), ()))
NT = (((1,), (1,)), ((), ()))
TN = (((0,), (0,)), ((), ()))


def dot(a, b, dims):
    return lax.dot_general(a, b, dims, preferred_element_type=F32)


def call(body, outs, scratch=(), flops=0, fetched=False, limit=16 * 2**20):
    size = sum(o.size * o.dtype.itemsize for o in jax.tree.leaves(outs))
    space = pl.BlockSpec(memory_space=pltpu.VMEM)
    inputs = pl.BlockSpec(memory_space=pltpu.HBM) if fetched else space

    def run(*args):
        if fetched:
            args = [pltpu.with_memory_space_constraint(x, pltpu.HBM) for x in args]
        return pl.pallas_call(
            body,
            out_shape=outs,
            in_specs=[inputs] * len(args),
            out_specs=jax.tree.map(lambda _: space, outs),
            scratch_shapes=scratch,
            compiler_params=pltpu.CompilerParams(vmem_limit_bytes=limit),
            cost_estimate=pl.CostEstimate(flops=flops, bytes_accessed=2 * size, transcendentals=0),
        )(*args)

    return run


def sds(shape, dtype):
    return jax.ShapeDtypeStruct(shape, dtype)


def aligned(index, size, unit):
    return pl.ds(pl.multiple_of(index * size, unit), size)


def pack(block):
    rows = block.shape[0] // 2
    return jnp.concatenate([block[:rows], block[rows:]], axis=1)


def unpack(block, width):
    return jnp.concatenate([block[:, :width], block[:, width : 2 * width]], axis=0)


def load_body(w_hbm, ids_hbm, weight_hbm, cot_hbm, hid_hbm, *refs):
    same_ref, cross_ref, same_hid_ref, cross_hid_ref, ids_ref, weight_ref, cot_ref, hid_ref, sems = refs
    h = lax.axis_index("h")
    rows, half = same_ref.shape
    same = w_hbm.at[:, aligned(h, half, 128)]
    cross = w_hbm.at[:, aligned(1 - h, half, 128)]
    jobs = (
        (hid_hbm, hid_ref),
        (same, same_ref),
        (cross, cross_ref),
        (cross, cross_hid_ref.at[0:rows]),
        (same, same_hid_ref.at[0:rows]),
        (ids_hbm, ids_ref),
        (weight_hbm, weight_ref),
        (cot_hbm, cot_ref),
    )
    copies = [pltpu.make_async_copy(source, target, sems.at[i]) for i, (source, target) in enumerate(jobs)]
    for copy in copies:
        copy.start()
    copies[0].wait()
    packed = pack(hid_ref[...])
    same_hid_ref[rows:, 0 : packed.shape[1]] = packed
    cross_hid_ref[rows:, 0 : packed.shape[1]] = packed
    for copy in copies[1:]:
        copy.wait()


def route_body(experts, capacity, ids_ref, weight_ref, cot_ref, sent_ref, table_ref, index_ref):
    half = sent_ref.shape[1]
    ids = ids_ref[...]
    weights = weight_ref[...]
    tokens = ids.shape[1]
    row = lax.broadcasted_iota(jnp.int32, (tokens, tokens), 0)
    col = lax.broadcasted_iota(jnp.int32, (tokens, tokens), 1)
    earlier = jnp.where(row < col, 1.0, 0.0).astype(BF16)
    named = [jnp.sum(jnp.where(ids == e, 1.0, 0.0), axis=0, keepdims=True) for e in range(experts)]
    mixing = [jnp.sum(jnp.where(ids == e, weights, 0.0), axis=0, keepdims=True) for e in range(experts)]
    preceding = dot(jnp.concatenate(named, axis=0).astype(BF16), earlier, NN)
    slot = lax.broadcasted_iota(jnp.int32, (capacity, tokens), 0).astype(F32)
    chosen, combine = [], []
    index = jnp.full(ids.shape, -1.0, F32)
    for e in range(experts):
        rank = preceding[e : e + 1]
        match = jnp.where(rank == slot, 1.0, 0.0) * named[e]
        chosen.append(match)
        combine.append(match * mixing[e])
        index = jnp.where(ids == e, rank + float(e * capacity), index)
    index_ref[...] = index
    chosen = jnp.concatenate(chosen, axis=0)
    combine = jnp.concatenate(combine, axis=0)
    slots = chosen.shape[0]
    slot_weight = jnp.sum(combine, axis=1, keepdims=True)
    high = combine.astype(BF16)
    rest = combine - high.astype(F32)
    middle = rest.astype(BF16)
    table_ref[0:slots] = high
    table_ref[slots : 2 * slots] = middle
    table_ref[2 * slots : 3 * slots] = (rest - middle.astype(F32)).astype(BF16)
    gathered = dot(chosen.astype(BF16), cot_ref[...], NN)
    value = (gathered * slot_weight).astype(BF16)
    for g in range(2):
        sent_ref[g * slots : (g + 1) * slots] = value[:, g * half : (g + 1) * half]


def weight_grad_body(moves, groups, width, *refs):
    hidden_refs, (grad_ref, partner_ref, give_ref) = refs[:4], refs[4:7]
    sends, (hid_ref, total_ref) = refs[7 : 7 + len(moves)], refs[7 + len(moves) :]
    q, h, c = lax.axis_index("q"), lax.axis_index("h"), lax.axis_index("c")
    rows = sends[0].shape[0]
    slots = hid_ref.shape[0] // 4
    for ref, group in zip(hidden_refs, (h, 1 - h, 2 + h, 3 - h), strict=True):
        hid_ref[aligned(group, slots, 16), :] = unpack(ref[rows:], width)
    grads = jnp.concatenate([grad_ref[...], partner_ref[...]], axis=0)
    total_ref[...] = dot(hid_ref[...], grads, TN)
    for (dq, dh), send in zip(moves, sends, strict=True):
        target = (lax.rem(q + dq, groups) * 2 + lax.rem(h + dh, 2)) * 2 + c
        send[0:rows] = total_ref[aligned(target, rows, 8), :].astype(send.dtype)
    sends[1][rows:, 0 : 2 * width] = pack(give_ref[...])


def expert_body(moves, groups, width, *refs):
    count = len(moves)
    blocks = refs[: 2 * count]
    grad_ref, out_ref, keep_ref, give_ref, hid_ref, stage_ref = refs[2 * count :]
    q, h, c = lax.axis_index("q"), lax.axis_index("h"), lax.axis_index("c")
    slots = keep_ref.shape[0]
    rows = blocks[0].shape[0] - slots // 2
    for i, (dq, dh) in enumerate(moves):
        source = (lax.rem(q + (groups - dq), groups) * 2 + lax.rem(h + dh, 2)) * 2
        for side, core in ((0, c), (count, 1 - c)):
            stage_ref[aligned(source + core, rows, 8), :] = blocks[side + i][0:rows].astype(stage_ref.dtype)
    for i, group in enumerate((h, 1 - h)):
        hid_ref[aligned(group, slots, 16), :] = unpack(blocks[i][rows:], width)
    full = stage_ref[...].astype(BF16)
    out_ref[...] = dot(hid_ref[...], full, NN).astype(BF16)
    keep_ref[...] = dot(grad_ref[aligned(h, slots, 16), :], full, NT)
    give_ref[...] = dot(grad_ref[aligned(1 - h, slots, 16), :], full, NT).astype(BF16)


def combine_body(arrived_ref, table_ref, index_ref, cot_ref, layer_ref, route_ref):
    slots, half = arrived_ref.shape[0] // 2, arrived_ref.shape[1]
    scores = None
    for g in range(2):
        rows = arrived_ref[g * slots : (g + 1) * slots]
        mixed = dot(table_ref[...], jnp.concatenate([rows] * 3, axis=0), TN)
        layer_ref[:, g * half : (g + 1) * half] = mixed.astype(BF16)
        part = dot(rows, cot_ref[:, g * half : (g + 1) * half], NT)
        scores = part if scores is None else scores + part
    position = lax.broadcasted_iota(jnp.int32, scores.shape, 0).astype(F32)
    for k in range(index_ref.shape[0]):
        hit = position == index_ref[k : k + 1]
        route_ref[k : k + 1] = jnp.sum(jnp.where(hit, scores, 0.0), axis=0, keepdims=True)


def finish_body(moves, keep_ref, *refs):
    count = len(moves)
    terms, (hidden_ref, weight_ref) = refs[:count], refs[count:]
    h = lax.axis_index("h")
    rows, half = terms[0].shape
    given = unpack(terms[1][rows:], hidden_ref.shape[1])
    hidden_ref[...] = (keep_ref[...] + given.astype(F32)).astype(BF16)
    for side in range(2):
        total = None
        for (_, dh), term in zip(moves, terms, strict=True):
            if dh == side:
                value = term[0:rows].astype(F32)
                total = value if total is None else total + value
        weight_ref[:, aligned(h if side == 0 else 1 - h, half, 128)] = total


def local(route_ids, route_weights, hidden, down_weight, cotangent):
    groups = lax.axis_size("q")
    experts = lax.axis_size("ep")
    tokens, features = cotangent.shape
    capacity, width = hidden.shape[3], hidden.shape[4]
    rows = down_weight.shape[1]
    slots = experts * capacity
    choices = route_ids.shape[1]
    half = features // 2
    moves = [(0, 0), (0, 1)] + [(dq, dh) for dq in range(1, groups) for dh in range(2)]
    swap = [(0, 1), (1, 0)]

    def move(x, step):
        dq, dh = step
        pairs = [(a * 2 + b, (a + dq) % groups * 2 + (b + dh) % 2) for a in range(groups) for b in range(2)]
        return lax.ppermute(x, ("q", "h"), pairs)

    def swap_core(x):
        return lax.ppermute(x, "c", swap)

    def exchange(x):
        parts = x.reshape(2 * experts, capacity, half)
        return lax.all_to_all(parts, ("h", "ep"), split_axis=0, concat_axis=0, tiled=True).reshape(x.shape)

    plain = sds((rows, half), BF16)
    joined = sds((rows + slots // 2, half), BF16)
    parts = sds((2 * slots, half), BF16)
    same, cross, same_hid, cross_hid, ids, weights, cot = call(
        load_body,
        (plain, plain, joined, joined, sds((choices, tokens), route_ids.dtype), sds((choices, tokens), F32), sds(cotangent.shape, BF16)),
        [pltpu.VMEM((slots, width), BF16), pltpu.SemaphoreType.DMA((8,))],
        fetched=True,
        limit=LOAD_LIMIT,
    )(down_weight[0], route_ids.T, route_weights.T, cotangent, hidden.reshape(slots, width))

    blocks = [same_hid, move(cross_hid, moves[1])]
    blocks += [move(cross if step[1] else same, step) for i, step in enumerate(moves) if i > 1]
    blocks += [swap_core(b) for b in blocks]
    sent, table, index = call(
        functools.partial(route_body, experts, capacity),
        (parts, sds((3 * slots, tokens), BF16), sds((choices, tokens), F32)),
        flops=2 * slots * tokens * features,
    )(ids, weights, cot)
    grads = exchange(sent)
    partner_grads = swap_core(grads)

    given, keep, give = call(
        functools.partial(expert_body, moves, groups, width),
        (parts, sds((slots, width), F32), sds((slots, width), BF16)),
        [
            pltpu.VMEM((2 * slots, width), BF16),
            pltpu.VMEM((width, half), BF16 if rows % 16 == 0 else F32),
        ],
        flops=8 * slots * width * half,
    )(*blocks, grads)
    weight_terms = call(
        functools.partial(weight_grad_body, moves, groups, width),
        (sds((rows, half), F32), joined, *[plain] * (len(moves) - 2)),
        [pltpu.VMEM((4 * slots, width), BF16), pltpu.VMEM((width, half), F32)],
        flops=8 * slots * width * half,
    )(blocks[0], blocks[1], blocks[len(moves)], blocks[len(moves) + 1], grads, partner_grads, give)
    terms = [weight_terms[0]] + [move(weight_terms[i], step) for i, step in enumerate(moves) if i]

    arrived = exchange(given)

    layer_out, route_grad = call(
        combine_body, (sds((tokens, features), BF16), sds((choices, tokens), F32)), flops=8 * slots * tokens * features
    )(arrived, table, index, cot)

    hidden_grad, weight_grad = call(
        functools.partial(finish_body, moves),
        (sds((slots, width), BF16), sds((rows, features), F32)),
        flops=rows * features,
    )(keep, *terms)
    return layer_out, route_grad.T, hidden_grad.reshape(hidden.shape), weight_grad[None]


def solution(mesh):
    edp, ep = mesh.shape["edp"], mesh.shape["ep"]
    fine = Mesh(mesh.devices.reshape(edp // 4, 2, 2, ep), ("q", "h", "c", "ep"))
    group = ("q", "h", "c")
    tokens = P(group + ("ep",), None)
    slots = P(group, "ep", None, None, None)
    weights = P("ep", group, None)
    return jax.shard_map(
        local,
        mesh=fine,
        in_specs=(tokens, tokens, slots, weights, tokens),
        out_specs=(tokens, tokens, slots, weights),
        check_vma=False,
    )
```

```python
import functools

import jax
import jax.numpy as jnp
from jax import lax
from jax.experimental import pallas as pl
from jax.experimental.pallas import tpu as pltpu
from jax.sharding import Mesh
from jax.sharding import PartitionSpec as P


BF16 = jnp.bfloat16
F32 = jnp.float32
NN = (((1,), (0,)), ((), ()))
NT = (((1,), (1,)), ((), ()))
TN = (((0,), (0,)), ((), ()))


def dot(a, b, dims):
    return lax.dot_general(a, b, dims, preferred_element_type=F32)


def call(body, outs, scratch=(), flops=0, fetched=False, limit=16 * 2**20):
    size = sum(o.size * o.dtype.itemsize for o in jax.tree.leaves(outs))
    space = pl.BlockSpec(memory_space=pltpu.VMEM)
    inputs = pl.BlockSpec(memory_space=pltpu.HBM) if fetched else space

    def run(*args):
        if fetched:
            args = [pltpu.with_memory_space_constraint(x, pltpu.HBM) for x in args]
        return pl.pallas_call(
            body,
            out_shape=outs,
            in_specs=[inputs] * len(args),
            out_specs=jax.tree.map(lambda _: space, outs),
            scratch_shapes=scratch,
            compiler_params=pltpu.CompilerParams(vmem_limit_bytes=limit),
            cost_estimate=pl.CostEstimate(flops=flops, bytes_accessed=2 * size, transcendentals=0),
        )(*args)

    return run


def sds(shape, dtype):
    return jax.ShapeDtypeStruct(shape, dtype)


def aligned(index, size, unit):
    return pl.ds(pl.multiple_of(index * size, unit), size)


def pack(block):
    rows = block.shape[0] // 2
    return jnp.concatenate([block[:rows], block[rows:]], axis=1)


def unpack(block, width):
    return jnp.concatenate([block[:, :width], block[:, width : 2 * width]], axis=0)


def load_body(w_hbm, ids_hbm, weight_hbm, cot_hbm, hid_hbm, *refs):
    same_ref, cross_ref, same_hid_ref, cross_hid_ref, ids_ref, weight_ref, cot_ref, hid_ref, sems = refs
    h = lax.axis_index("h")
    rows, half = same_ref.shape
    same = w_hbm.at[:, aligned(h, half, 128)]
    cross = w_hbm.at[:, aligned(1 - h, half, 128)]
    jobs = (
        (hid_hbm, hid_ref),
        (same, same_ref),
        (cross, cross_ref),
        (cross, cross_hid_ref.at[0:rows]),
        (same, same_hid_ref.at[0:rows]),
        (ids_hbm, ids_ref),
        (weight_hbm, weight_ref),
        (cot_hbm, cot_ref),
    )
    copies = [pltpu.make_async_copy(source, target, sems.at[i]) for i, (source, target) in enumerate(jobs)]
    for copy in copies:
        copy.start()
    copies[0].wait()
    packed = pack(hid_ref[...])
    same_hid_ref[rows:, 0 : packed.shape[1]] = packed
    cross_hid_ref[rows:, 0 : packed.shape[1]] = packed
    for copy in copies[1:]:
        copy.wait()


def slot_tables(experts, capacity, ids, weights):
    tokens = ids.shape[1]
    row = lax.broadcasted_iota(jnp.int32, (tokens, tokens), 0)
    col = lax.broadcasted_iota(jnp.int32, (tokens, tokens), 1)
    earlier = jnp.where(row < col, 1.0, 0.0).astype(BF16)
    named = [jnp.sum(jnp.where(ids == e, 1.0, 0.0), axis=0, keepdims=True) for e in range(experts)]
    mixing = [jnp.sum(jnp.where(ids == e, weights, 0.0), axis=0, keepdims=True) for e in range(experts)]
    preceding = dot(jnp.concatenate(named, axis=0).astype(BF16), earlier, NN)
    slot = lax.broadcasted_iota(jnp.int32, (capacity, tokens), 0).astype(F32)
    chosen = [jnp.where(preceding[e : e + 1] == slot, 1.0, 0.0) * named[e] for e in range(experts)]
    combine = jnp.concatenate([match * mix for match, mix in zip(chosen, mixing, strict=True)], axis=0)
    return preceding, jnp.concatenate(chosen, axis=0), combine


def route_body(experts, capacity, ids_ref, weight_ref, cot_ref, sent_ref):
    half = sent_ref.shape[1]
    _, chosen, combine = slot_tables(experts, capacity, ids_ref[...], weight_ref[...])
    slots = chosen.shape[0]
    slot_weight = jnp.sum(combine, axis=1, keepdims=True)
    gathered = dot(chosen.astype(BF16), cot_ref[...], NN)
    value = (gathered * slot_weight).astype(BF16)
    for g in range(2):
        sent_ref[g * slots : (g + 1) * slots] = value[:, g * half : (g + 1) * half]


def tables_body(experts, capacity, ids_ref, weight_ref, table_ref, index_ref):
    ids = ids_ref[...]
    preceding, _, combine = slot_tables(experts, capacity, ids, weight_ref[...])
    index = jnp.full(ids.shape, -1.0, F32)
    for e in range(experts):
        index = jnp.where(ids == e, preceding[e : e + 1] + float(e * capacity), index)
    index_ref[...] = index
    slots = combine.shape[0]
    high = combine.astype(BF16)
    rest = combine - high.astype(F32)
    middle = rest.astype(BF16)
    table_ref[0:slots] = high
    table_ref[slots : 2 * slots] = middle
    table_ref[2 * slots : 3 * slots] = (rest - middle.astype(F32)).astype(BF16)


def peer(index, step, count):
    if count & (count - 1) == 0:
        return index ^ step
    return lax.rem(index + step, count)


def origin(index, step, count):
    return peer(index, step if count & (count - 1) == 0 else (count - step) % count, count)


def join_body(own_ref, other_ref, *pieces):
    h, s = lax.axis_index("h"), lax.axis_index("ep")
    count = len(pieces)
    unit = own_ref.shape[0] // count
    for step, piece in enumerate(pieces):
        rows = aligned(peer(s, step, count), unit, 16)
        piece[aligned(h, unit, 16), :] = own_ref[rows, :]
        piece[aligned(1 - h, unit, 16), :] = other_ref[rows, :]


def weight_grad_body(moves, groups, width, *refs):
    hidden_refs, (grad_ref, partner_ref, give_ref) = refs[:4], refs[4:7]
    sends, (hid_ref, total_ref) = refs[7 : 7 + len(moves)], refs[7 + len(moves) :]
    q, h, c = lax.axis_index("q"), lax.axis_index("h"), lax.axis_index("c")
    rows = sends[0].shape[0]
    slots = hid_ref.shape[0] // 4
    for ref, group in zip(hidden_refs, (h, 1 - h, 2 + h, 3 - h), strict=True):
        hid_ref[aligned(group, slots, 16), :] = unpack(ref[rows:], width)
    grads = jnp.concatenate([grad_ref[...], partner_ref[...]], axis=0)
    total_ref[...] = dot(hid_ref[...], grads, TN)
    for (dq, dh), send in zip(moves, sends, strict=True):
        target = (lax.rem(q + dq, groups) * 2 + lax.rem(h + dh, 2)) * 2 + c
        send[0:rows] = total_ref[aligned(target, rows, 8), :].astype(send.dtype)
    sends[1][rows:, 0 : 2 * width] = pack(give_ref[...])


def expert_body(moves, groups, width, *refs):
    count = len(moves)
    blocks = refs[: 2 * count]
    grad_ref, own_ref, other_ref, keep_ref, give_ref, hid_ref, stage_ref = refs[2 * count :]
    q, h, c = lax.axis_index("q"), lax.axis_index("h"), lax.axis_index("c")
    slots = keep_ref.shape[0]
    rows = blocks[0].shape[0] - slots // 2
    for i, (dq, dh) in enumerate(moves):
        source = (lax.rem(q + (groups - dq), groups) * 2 + lax.rem(h + dh, 2)) * 2
        for side, core in ((0, c), (count, 1 - c)):
            stage_ref[aligned(source + core, rows, 8), :] = blocks[side + i][0:rows].astype(stage_ref.dtype)
    for i in range(2):
        hid_ref[i * slots : (i + 1) * slots] = unpack(blocks[i][rows:], width)
    full = stage_ref[...].astype(BF16)
    out = dot(hid_ref[...], full, NN).astype(BF16)
    own_ref[...] = out[0:slots]
    other_ref[...] = out[slots:]
    keep_ref[...] = dot(grad_ref[aligned(h, slots, 16), :], full, NT)
    give_ref[...] = dot(grad_ref[aligned(1 - h, slots, 16), :], full, NT).astype(BF16)


def combine_body(table_ref, index_ref, cot_ref, *refs):
    pieces, (layer_ref, route_ref, arrived_ref) = refs[:-3], refs[-3:]
    count = len(pieces)
    unit = pieces[0].shape[0] // 2
    slots, half = count * unit, arrived_ref.shape[1]
    s = lax.axis_index("ep")
    for step, piece in enumerate(pieces):
        source = origin(s, step, count)
        for g in range(2):
            arrived_ref[aligned(g * count + source, unit, 16), :] = piece[g * unit : (g + 1) * unit]
    scores = None
    for g in range(2):
        rows = arrived_ref[g * slots : (g + 1) * slots]
        mixed = dot(table_ref[...], jnp.concatenate([rows] * 3, axis=0), TN)
        layer_ref[:, g * half : (g + 1) * half] = mixed.astype(BF16)
        part = dot(rows, cot_ref[:, g * half : (g + 1) * half], NT)
        scores = part if scores is None else scores + part
    position = lax.broadcasted_iota(jnp.int32, scores.shape, 0).astype(F32)
    for k in range(index_ref.shape[0]):
        hit = position == index_ref[k : k + 1]
        route_ref[k : k + 1] = jnp.sum(jnp.where(hit, scores, 0.0), axis=0, keepdims=True)


def finish_body(moves, keep_ref, *refs):
    count = len(moves)
    terms, (hidden_ref, weight_ref) = refs[:count], refs[count:]
    h = lax.axis_index("h")
    rows, half = terms[0].shape
    given = unpack(terms[1][rows:], hidden_ref.shape[1])
    hidden_ref[...] = (keep_ref[...] + given.astype(F32)).astype(BF16)
    for side in range(2):
        total = None
        for (_, dh), term in zip(moves, terms, strict=True):
            if dh == side:
                value = term[0:rows].astype(F32)
                total = value if total is None else total + value
        weight_ref[:, aligned(h if side == 0 else 1 - h, half, 128)] = total


def local(route_ids, route_weights, hidden, down_weight, cotangent):
    groups = lax.axis_size("q")
    experts = lax.axis_size("ep")
    tokens, features = cotangent.shape
    capacity, width = hidden.shape[3], hidden.shape[4]
    rows = down_weight.shape[1]
    slots = experts * capacity
    choices = route_ids.shape[1]
    half = features // 2
    moves = [(0, 0), (0, 1)] + [(dq, dh) for dq in range(1, groups) for dh in range(2)]
    swap = [(0, 1), (1, 0)]

    def move(x, step):
        dq, dh = step
        pairs = [(a * 2 + b, (a + dq) % groups * 2 + (b + dh) % 2) for a in range(groups) for b in range(2)]
        return lax.ppermute(x, ("q", "h"), pairs)

    def swap_core(x):
        return lax.ppermute(x, "c", swap)

    def exchange(x):
        parts = x.reshape(2 * experts, capacity, half)
        return lax.all_to_all(parts, ("h", "ep"), split_axis=0, concat_axis=0, tiled=True).reshape(x.shape)

    plain = sds((rows, half), BF16)
    joined = sds((rows + slots // 2, half), BF16)
    parts = sds((2 * slots, half), BF16)
    part = sds((slots, half), BF16)
    same, cross, same_hid, cross_hid, ids, weights, cot = call(
        load_body,
        (plain, plain, joined, joined, sds((choices, tokens), route_ids.dtype), sds((choices, tokens), F32), sds(cotangent.shape, BF16)),
        [pltpu.VMEM((slots, width), BF16), pltpu.SemaphoreType.DMA((8,))],
        fetched=True,
    )(down_weight[0], route_ids.T, route_weights.T, cotangent, hidden.reshape(slots, width))

    blocks = [same_hid, move(cross_hid, moves[1])]
    blocks += [move(cross if step[1] else same, step) for i, step in enumerate(moves) if i > 1]
    blocks += [swap_core(b) for b in blocks]
    sent = call(
        functools.partial(route_body, experts, capacity), parts, flops=2 * slots * tokens * features
    )(ids, weights, cot)
    table, index = call(
        functools.partial(tables_body, experts, capacity),
        (sds((3 * slots, tokens), BF16), sds((choices, tokens), F32)),
        flops=2 * tokens * tokens * experts,
    )(ids, weights)
    grads = exchange(sent)
    partner_grads = swap_core(grads)

    own_out, other_out, keep, give = call(
        functools.partial(expert_body, moves, groups, width),
        (part, part, sds((slots, width), F32), sds((slots, width), BF16)),
        [
            pltpu.VMEM((2 * slots, width), BF16),
            pltpu.VMEM((width, half), BF16 if rows % 16 == 0 else F32),
        ],
        flops=8 * slots * width * half,
    )(*blocks, grads)
    other_half = lax.ppermute(other_out, "h", swap)

    weight_terms = call(
        functools.partial(weight_grad_body, moves, groups, width),
        (sds((rows, half), F32), joined, *[plain] * (len(moves) - 2)),
        [pltpu.VMEM((4 * slots, width), BF16), pltpu.VMEM((width, half), F32)],
        flops=8 * slots * width * half,
    )(blocks[0], blocks[1], blocks[len(moves)], blocks[len(moves) + 1], grads, partner_grads, give)
    terms = [weight_terms[0]] + [move(weight_terms[i], step) for i, step in enumerate(moves) if i]

    parcels = call(join_body, (sds((2 * capacity, half), BF16),) * experts, flops=slots)(own_out, other_half)
    arrived = [parcels[0]]
    for step in range(1, experts):
        pairs = [(e, int(peer(e, step, experts))) for e in range(experts)]
        arrived.append(lax.ppermute(parcels[step], "ep", pairs))

    layer_out, route_grad = call(
        combine_body,
        (sds((tokens, features), BF16), sds((choices, tokens), F32)),
        [pltpu.VMEM((2 * slots, half), BF16)],
        flops=8 * slots * tokens * features,
    )(table, index, cot, *arrived)

    hidden_grad, weight_grad = call(
        functools.partial(finish_body, moves),
        (sds((slots, width), BF16), sds((rows, features), F32)),
        flops=rows * features,
    )(keep, *terms)
    return layer_out, route_grad.T, hidden_grad.reshape(hidden.shape), weight_grad[None]


def solution(mesh):
    edp, ep = mesh.shape["edp"], mesh.shape["ep"]
    fine = Mesh(mesh.devices.reshape(edp // 4, 2, 2, ep), ("q", "h", "c", "ep"))
    group = ("q", "h", "c")
    tokens = P(group + ("ep",), None)
    slots = P(group, "ep", None, None, None)
    weights = P("ep", group, None)
    return jax.shard_map(
        local,
        mesh=fine,
        in_specs=(tokens, tokens, slots, weights, tokens),
        out_specs=(tokens, tokens, slots, weights),
        check_vma=False,
    )
```

```python
import functools

import jax
import jax.numpy as jnp
from jax import lax
from jax.experimental import pallas as pl
from jax.experimental.pallas import tpu as pltpu
from jax.sharding import Mesh
from jax.sharding import PartitionSpec as P


BF16 = jnp.bfloat16
F32 = jnp.float32
NN = (((1,), (0,)), ((), ()))
NT = (((1,), (1,)), ((), ()))
TN = (((0,), (0,)), ((), ()))


def dot(a, b, dims):
    return lax.dot_general(a, b, dims, preferred_element_type=F32)


def call(body, outs, scratch=(), flops=0, fetched=False, written=False, limit=16 * 2**20):
    size = sum(o.size * o.dtype.itemsize for o in jax.tree.leaves(outs))
    space = pl.BlockSpec(memory_space=pltpu.VMEM)
    inputs = pl.BlockSpec(memory_space=pltpu.HBM) if fetched else space
    outputs = pl.BlockSpec(memory_space=pltpu.HBM) if written else space

    def run(*args):
        if fetched:
            args = [pltpu.with_memory_space_constraint(x, pltpu.HBM) for x in args]
        return pl.pallas_call(
            body,
            out_shape=outs,
            in_specs=[inputs] * len(args),
            out_specs=jax.tree.map(lambda _: outputs, outs),
            scratch_shapes=scratch,
            compiler_params=pltpu.CompilerParams(vmem_limit_bytes=limit),
            cost_estimate=pl.CostEstimate(flops=flops, bytes_accessed=2 * size, transcendentals=0),
        )(*args)

    return run


def sds(shape, dtype):
    return jax.ShapeDtypeStruct(shape, dtype)


def aligned(index, size, unit):
    return pl.ds(pl.multiple_of(index * size, unit), size)


def pack(block):
    rows = block.shape[0] // 2
    return jnp.concatenate([block[:rows], block[rows:]], axis=1)


def unpack(block, width):
    return jnp.concatenate([block[:, :width], block[:, width : 2 * width]], axis=0)


def load_body(w_hbm, ids_hbm, weight_hbm, cot_hbm, hid_hbm, *refs):
    same_ref, cross_ref, same_hid_ref, cross_hid_ref, ids_ref, weight_ref, cot_ref, hid_ref, sems = refs
    h = lax.axis_index("h")
    rows, half = same_ref.shape
    same = w_hbm.at[:, aligned(h, half, 128)]
    cross = w_hbm.at[:, aligned(1 - h, half, 128)]
    jobs = (
        (hid_hbm, hid_ref),
        (same, same_ref),
        (cross, cross_ref),
        (cross, cross_hid_ref.at[0:rows]),
        (same, same_hid_ref.at[0:rows]),
        (ids_hbm, ids_ref),
        (weight_hbm, weight_ref),
        (cot_hbm, cot_ref),
    )
    copies = [pltpu.make_async_copy(source, target, sems.at[i]) for i, (source, target) in enumerate(jobs)]
    for copy in copies:
        copy.start()
    copies[0].wait()
    packed = pack(hid_ref[...])
    same_hid_ref[rows:, 0 : packed.shape[1]] = packed
    cross_hid_ref[rows:, 0 : packed.shape[1]] = packed
    for copy in copies[1:]:
        copy.wait()


def slot_tables(experts, capacity, ids, weights):
    tokens = ids.shape[1]
    row = lax.broadcasted_iota(jnp.int32, (tokens, tokens), 0)
    col = lax.broadcasted_iota(jnp.int32, (tokens, tokens), 1)
    earlier = jnp.where(row < col, 1.0, 0.0).astype(BF16)
    named = [jnp.sum(jnp.where(ids == e, 1.0, 0.0), axis=0, keepdims=True) for e in range(experts)]
    mixing = [jnp.sum(jnp.where(ids == e, weights, 0.0), axis=0, keepdims=True) for e in range(experts)]
    preceding = dot(jnp.concatenate(named, axis=0).astype(BF16), earlier, NN)
    slot = lax.broadcasted_iota(jnp.int32, (capacity, tokens), 0).astype(F32)
    chosen = [jnp.where(preceding[e : e + 1] == slot, 1.0, 0.0) * named[e] for e in range(experts)]
    combine = jnp.concatenate([match * mix for match, mix in zip(chosen, mixing, strict=True)], axis=0)
    return preceding, jnp.concatenate(chosen, axis=0), combine


def route_body(experts, capacity, ids_ref, weight_ref, cot_ref, sent_ref):
    half = sent_ref.shape[1]
    _, chosen, combine = slot_tables(experts, capacity, ids_ref[...], weight_ref[...])
    slots = chosen.shape[0]
    slot_weight = jnp.sum(combine, axis=1, keepdims=True)
    gathered = dot(chosen.astype(BF16), cot_ref[...], NN)
    value = (gathered * slot_weight).astype(BF16)
    for g in range(2):
        sent_ref[g * slots : (g + 1) * slots] = value[:, g * half : (g + 1) * half]


def tables_body(experts, capacity, ids_ref, weight_ref, table_ref, index_ref):
    ids = ids_ref[...]
    preceding, _, combine = slot_tables(experts, capacity, ids, weight_ref[...])
    index = jnp.full(ids.shape, -1.0, F32)
    for e in range(experts):
        index = jnp.where(ids == e, preceding[e : e + 1] + float(e * capacity), index)
    index_ref[...] = index
    slots = combine.shape[0]
    high = combine.astype(BF16)
    rest = combine - high.astype(F32)
    middle = rest.astype(BF16)
    table_ref[0:slots] = high
    table_ref[slots : 2 * slots] = middle
    table_ref[2 * slots : 3 * slots] = (rest - middle.astype(F32)).astype(BF16)


def peer(index, step, count):
    if count & (count - 1) == 0:
        return index ^ step
    return lax.rem(index + step, count)


def origin(index, step, count):
    return peer(index, step if count & (count - 1) == 0 else (count - step) % count, count)


def join_body(own_ref, other_ref, *pieces):
    h, s = lax.axis_index("h"), lax.axis_index("ep")
    count = len(pieces)
    unit = own_ref.shape[0] // count
    for step, piece in enumerate(pieces):
        rows = aligned(peer(s, step, count), unit, 16)
        piece[aligned(h, unit, 16), :] = own_ref[rows, :]
        piece[aligned(1 - h, unit, 16), :] = other_ref[rows, :]


def weight_grad_body(moves, groups, width, *refs):
    hidden_refs, (grad_ref, partner_ref, give_ref) = refs[:4], refs[4:7]
    sends, (hid_ref, total_ref) = refs[7 : 7 + len(moves)], refs[7 + len(moves) :]
    q, h, c = lax.axis_index("q"), lax.axis_index("h"), lax.axis_index("c")
    rows = sends[0].shape[0]
    slots = hid_ref.shape[0] // 4
    for ref, group in zip(hidden_refs, (h, 1 - h, 2 + h, 3 - h), strict=True):
        hid_ref[aligned(group, slots, 16), :] = unpack(ref[rows:], width)
    grads = jnp.concatenate([grad_ref[...], partner_ref[...]], axis=0)
    total_ref[...] = dot(hid_ref[...], grads, TN)
    for (dq, dh), send in zip(moves, sends, strict=True):
        target = (lax.rem(q + dq, groups) * 2 + lax.rem(h + dh, 2)) * 2 + c
        send[0:rows] = total_ref[aligned(target, rows, 8), :].astype(send.dtype)
    sends[1][rows:, 0 : 2 * width] = pack(give_ref[...])


def expert_body(moves, groups, width, *refs):
    count = len(moves)
    blocks = refs[: 2 * count]
    grad_ref, own_ref, other_ref, keep_ref, give_ref, hid_ref, stage_ref = refs[2 * count :]
    q, h, c = lax.axis_index("q"), lax.axis_index("h"), lax.axis_index("c")
    slots = keep_ref.shape[0]
    rows = blocks[0].shape[0] - slots // 2
    for i, (dq, dh) in enumerate(moves):
        source = (lax.rem(q + (groups - dq), groups) * 2 + lax.rem(h + dh, 2)) * 2
        for side, core in ((0, c), (count, 1 - c)):
            stage_ref[aligned(source + core, rows, 8), :] = blocks[side + i][0:rows].astype(stage_ref.dtype)
    for i in range(2):
        hid_ref[i * slots : (i + 1) * slots] = unpack(blocks[i][rows:], width)
    full = stage_ref[...].astype(BF16)
    out = dot(hid_ref[...], full, NN).astype(BF16)
    own_ref[...] = out[0:slots]
    other_ref[...] = out[slots:]
    keep_ref[...] = dot(grad_ref[aligned(h, slots, 16), :], full, NT)
    give_ref[...] = dot(grad_ref[aligned(1 - h, slots, 16), :], full, NT).astype(BF16)


def finish_body(moves, experts, keep_ref, table_ref, index_ref, cot_ref, *refs):
    count = len(moves)
    terms, pieces = refs[:count], refs[count : count + experts]
    layer_hbm, route_hbm, hidden_hbm, weight_hbm, layer_ref, route_ref, hidden_ref, weight_ref, arrived_ref, sems = refs[count + experts :]
    h, s = lax.axis_index("h"), lax.axis_index("ep")
    rows, half = terms[0].shape
    copies = []

    def put(source, target):
        copies.append(pltpu.make_async_copy(source, target, sems.at[len(copies)]))
        copies[-1].start()

    for side in range(2):
        total = None
        for (_, dh), term in zip(moves, terms, strict=True):
            if dh == side:
                value = term[0:rows].astype(F32)
                total = value if total is None else total + value
        weight_ref[:, aligned(h if side == 0 else 1 - h, half, 128)] = total
    put(weight_ref, weight_hbm)
    given = unpack(terms[1][rows:], hidden_ref.shape[1])
    hidden_ref[...] = (keep_ref[...] + given.astype(F32)).astype(BF16)
    put(hidden_ref, hidden_hbm)
    unit = pieces[0].shape[0] // 2
    slots = experts * unit
    for step, piece in enumerate(pieces):
        source = origin(s, step, experts)
        for g in range(2):
            arrived_ref[aligned(g * experts + source, unit, 16), :] = piece[g * unit : (g + 1) * unit]
    scores = None
    for g in range(2):
        block = arrived_ref[g * slots : (g + 1) * slots]
        mixed = dot(table_ref[...], jnp.concatenate([block] * 3, axis=0), TN)
        layer_ref[g] = mixed.astype(BF16)
        put(layer_ref.at[g], layer_hbm.at[:, pl.ds(g * half, half)])
        part = dot(block, cot_ref[:, g * half : (g + 1) * half], NT)
        scores = part if scores is None else scores + part
    position = lax.broadcasted_iota(jnp.int32, scores.shape, 0).astype(F32)
    for k in range(index_ref.shape[0]):
        hit = position == index_ref[k : k + 1]
        route_ref[k : k + 1] = jnp.sum(jnp.where(hit, scores, 0.0), axis=0, keepdims=True)
    put(route_ref, route_hbm)
    for copy in copies:
        copy.wait()


def local(route_ids, route_weights, hidden, down_weight, cotangent):
    groups = lax.axis_size("q")
    experts = lax.axis_size("ep")
    tokens, features = cotangent.shape
    capacity, width = hidden.shape[3], hidden.shape[4]
    rows = down_weight.shape[1]
    slots = experts * capacity
    choices = route_ids.shape[1]
    half = features // 2
    moves = [(0, 0), (0, 1)] + [(dq, dh) for dq in range(1, groups) for dh in range(2)]
    swap = [(0, 1), (1, 0)]

    def move(x, step):
        dq, dh = step
        pairs = [(a * 2 + b, (a + dq) % groups * 2 + (b + dh) % 2) for a in range(groups) for b in range(2)]
        return lax.ppermute(x, ("q", "h"), pairs)

    def swap_core(x):
        return lax.ppermute(x, "c", swap)

    def exchange(x):
        parts = x.reshape(2 * experts, capacity, half)
        return lax.all_to_all(parts, ("h", "ep"), split_axis=0, concat_axis=0, tiled=True).reshape(x.shape)

    plain = sds((rows, half), BF16)
    joined = sds((rows + slots // 2, half), BF16)
    parts = sds((2 * slots, half), BF16)
    part = sds((slots, half), BF16)
    same, cross, same_hid, cross_hid, ids, weights, cot = call(
        load_body,
        (plain, plain, joined, joined, sds((choices, tokens), route_ids.dtype), sds((choices, tokens), F32), sds(cotangent.shape, BF16)),
        [pltpu.VMEM((slots, width), BF16), pltpu.SemaphoreType.DMA((8,))],
        fetched=True,
    )(down_weight[0], route_ids.T, route_weights.T, cotangent, hidden.reshape(slots, width))

    blocks = [same_hid, move(cross_hid, moves[1])]
    blocks += [move(cross if step[1] else same, step) for i, step in enumerate(moves) if i > 1]
    blocks += [swap_core(b) for b in blocks]
    sent = call(
        functools.partial(route_body, experts, capacity), parts, flops=2 * slots * tokens * features
    )(ids, weights, cot)
    table, index = call(
        functools.partial(tables_body, experts, capacity),
        (sds((3 * slots, tokens), BF16), sds((choices, tokens), F32)),
        flops=2 * tokens * tokens * experts,
    )(ids, weights)
    grads = exchange(sent)
    partner_grads = swap_core(grads)

    own_out, other_out, keep, give = call(
        functools.partial(expert_body, moves, groups, width),
        (part, part, sds((slots, width), F32), sds((slots, width), BF16)),
        [
            pltpu.VMEM((2 * slots, width), BF16),
            pltpu.VMEM((width, half), BF16 if rows % 16 == 0 else F32),
        ],
        flops=8 * slots * width * half,
    )(*blocks, grads)
    other_half = lax.ppermute(other_out, "h", swap)

    weight_terms = call(
        functools.partial(weight_grad_body, moves, groups, width),
        (sds((rows, half), F32), joined, *[plain] * (len(moves) - 2)),
        [pltpu.VMEM((4 * slots, width), BF16), pltpu.VMEM((width, half), F32)],
        flops=8 * slots * width * half,
    )(blocks[0], blocks[1], blocks[len(moves)], blocks[len(moves) + 1], grads, partner_grads, give)
    terms = [weight_terms[0]] + [move(weight_terms[i], step) for i, step in enumerate(moves) if i]

    parcels = call(join_body, (sds((2 * capacity, half), BF16),) * experts, flops=slots)(own_out, other_half)
    arrived = [parcels[0]]
    for step in range(1, experts):
        pairs = [(e, int(peer(e, step, experts))) for e in range(experts)]
        arrived.append(lax.ppermute(parcels[step], "ep", pairs))

    outs = (
        sds((tokens, features), BF16),
        sds((choices, tokens), F32),
        sds((slots, width), BF16),
        sds((rows, features), F32),
    )
    layer_out, route_grad, hidden_grad, weight_grad = call(
        functools.partial(finish_body, moves, experts),
        outs,
        [
            pltpu.VMEM((2, tokens, half), BF16),
            pltpu.VMEM((choices, tokens), F32),
            pltpu.VMEM((slots, width), BF16),
            pltpu.VMEM((rows, features), F32),
            pltpu.VMEM((2 * slots, half), BF16),
            pltpu.SemaphoreType.DMA((5,)),
        ],
        flops=8 * slots * tokens * features,
        written=True,
    )(keep, table, index, cot, *terms, *arrived)
    return layer_out, route_grad.T, hidden_grad.reshape(hidden.shape), weight_grad[None]


def solution(mesh):
    edp, ep = mesh.shape["edp"], mesh.shape["ep"]
    fine = Mesh(mesh.devices.reshape(edp // 4, 2, 2, ep), ("q", "h", "c", "ep"))
    group = ("q", "h", "c")
    tokens = P(group + ("ep",), None)
    slots = P(group, "ep", None, None, None)
    weights = P("ep", group, None)
    return jax.shard_map(
        local,
        mesh=fine,
        in_specs=(tokens, tokens, slots, weights, tokens),
        out_specs=(tokens, tokens, slots, weights),
        check_vma=False,
    )
```

```python
import functools

import jax
import jax.numpy as jnp
from jax import lax
from jax.experimental import pallas as pl
from jax.experimental.pallas import tpu as pltpu
from jax.sharding import Mesh
from jax.sharding import PartitionSpec as P


BF16 = jnp.bfloat16
F32 = jnp.float32
NN = (((1,), (0,)), ((), ()))
NT = (((1,), (1,)), ((), ()))
TN = (((0,), (0,)), ((), ()))


def dot(a, b, dims):
    return lax.dot_general(a, b, dims, preferred_element_type=F32)


def call(body, outs, scratch=(), flops=0, fetched=False, limit=16 * 2**20):
    size = sum(o.size * o.dtype.itemsize for o in jax.tree.leaves(outs))
    space = pl.BlockSpec(memory_space=pltpu.VMEM)
    inputs = pl.BlockSpec(memory_space=pltpu.HBM) if fetched else space

    def run(*args):
        if fetched:
            args = [pltpu.with_memory_space_constraint(x, pltpu.HBM) for x in args]
        return pl.pallas_call(
            body,
            out_shape=outs,
            in_specs=[inputs] * len(args),
            out_specs=jax.tree.map(lambda _: space, outs),
            scratch_shapes=scratch,
            compiler_params=pltpu.CompilerParams(vmem_limit_bytes=limit),
            cost_estimate=pl.CostEstimate(flops=flops, bytes_accessed=2 * size, transcendentals=0),
        )(*args)

    return run


def sds(shape, dtype):
    return jax.ShapeDtypeStruct(shape, dtype)


def aligned(index, size, unit):
    return pl.ds(pl.multiple_of(index * size, unit), size)


def pack(block):
    rows = block.shape[0] // 2
    return jnp.concatenate([block[:rows], block[rows:]], axis=1)


def unpack(block, width):
    return jnp.concatenate([block[:, :width], block[:, width : 2 * width]], axis=0)


def load_body(w_hbm, ids_hbm, weight_hbm, cot_hbm, hid_hbm, *refs):
    same_ref, cross_ref, same_hid_ref, cross_hid_ref, ids_ref, weight_ref, cot_ref, hid_ref, sems = refs
    h = lax.axis_index("h")
    rows, half = same_ref.shape
    same = w_hbm.at[:, aligned(h, half, 128)]
    cross = w_hbm.at[:, aligned(1 - h, half, 128)]
    jobs = (
        (hid_hbm, hid_ref),
        (same, same_ref),
        (cross, cross_ref),
        (cross, cross_hid_ref.at[0:rows]),
        (same, same_hid_ref.at[0:rows]),
        (ids_hbm, ids_ref),
        (weight_hbm, weight_ref),
        (cot_hbm, cot_ref),
    )
    copies = [pltpu.make_async_copy(source, target, sems.at[i]) for i, (source, target) in enumerate(jobs)]
    for copy in copies:
        copy.start()
    copies[0].wait()
    packed = pack(hid_ref[...])
    same_hid_ref[rows:, 0 : packed.shape[1]] = packed
    cross_hid_ref[rows:, 0 : packed.shape[1]] = packed
    for copy in copies[1:]:
        copy.wait()


def slot_tables(experts, capacity, ids, weights):
    tokens = ids.shape[1]
    row = lax.broadcasted_iota(jnp.int32, (tokens, tokens), 0)
    col = lax.broadcasted_iota(jnp.int32, (tokens, tokens), 1)
    earlier = jnp.where(row < col, 1.0, 0.0).astype(BF16)
    named = [jnp.sum(jnp.where(ids == e, 1.0, 0.0), axis=0, keepdims=True) for e in range(experts)]
    mixing = [jnp.sum(jnp.where(ids == e, weights, 0.0), axis=0, keepdims=True) for e in range(experts)]
    preceding = dot(jnp.concatenate(named, axis=0).astype(BF16), earlier, NN)
    slot = lax.broadcasted_iota(jnp.int32, (capacity, tokens), 0).astype(F32)
    chosen = [jnp.where(preceding[e : e + 1] == slot, 1.0, 0.0) * named[e] for e in range(experts)]
    combine = jnp.concatenate([match * mix for match, mix in zip(chosen, mixing, strict=True)], axis=0)
    return preceding, jnp.concatenate(chosen, axis=0), combine


def route_body(experts, capacity, ids_ref, weight_ref, cot_ref, sent_ref):
    half = sent_ref.shape[1]
    _, chosen, combine = slot_tables(experts, capacity, ids_ref[...], weight_ref[...])
    slots = chosen.shape[0]
    slot_weight = jnp.sum(combine, axis=1, keepdims=True)
    gathered = dot(chosen.astype(BF16), cot_ref[...], NN)
    value = (gathered * slot_weight).astype(BF16)
    for g in range(2):
        sent_ref[g * slots : (g + 1) * slots] = value[:, g * half : (g + 1) * half]


def tables_body(experts, capacity, ids_ref, weight_ref, table_ref, index_ref):
    ids = ids_ref[...]
    preceding, _, combine = slot_tables(experts, capacity, ids, weight_ref[...])
    index = jnp.full(ids.shape, -1.0, F32)
    for e in range(experts):
        index = jnp.where(ids == e, preceding[e : e + 1] + float(e * capacity), index)
    index_ref[...] = index
    slots = combine.shape[0]
    high = combine.astype(BF16)
    rest = combine - high.astype(F32)
    middle = rest.astype(BF16)
    table_ref[0:slots] = high
    table_ref[slots : 2 * slots] = middle
    table_ref[2 * slots : 3 * slots] = (rest - middle.astype(F32)).astype(BF16)


def peer(index, step, count):
    if count & (count - 1) == 0:
        return index ^ step
    return lax.rem(index + step, count)


def origin(index, step, count):
    return peer(index, step if count & (count - 1) == 0 else (count - step) % count, count)


def join_body(own_ref, other_ref, *pieces):
    h, s = lax.axis_index("h"), lax.axis_index("ep")
    count = len(pieces)
    unit = own_ref.shape[0] // count
    for step, piece in enumerate(pieces):
        rows = aligned(peer(s, step, count), unit, 16)
        piece[aligned(h, unit, 16), :] = own_ref[rows, :]
        piece[aligned(1 - h, unit, 16), :] = other_ref[rows, :]


def weight_grad_body(moves, groups, width, *refs):
    hidden_refs, (grad_ref, partner_ref, give_ref) = refs[:4], refs[4:7]
    sends, (hid_ref, total_ref) = refs[7 : 7 + len(moves)], refs[7 + len(moves) :]
    q, h, c = lax.axis_index("q"), lax.axis_index("h"), lax.axis_index("c")
    rows = sends[0].shape[0]
    slots = hid_ref.shape[0] // 4
    for ref, group in zip(hidden_refs, (h, 1 - h, 2 + h, 3 - h), strict=True):
        hid_ref[aligned(group, slots, 16), :] = unpack(ref[rows:], width)
    grads = jnp.concatenate([grad_ref[...], partner_ref[...]], axis=0)
    total_ref[...] = dot(hid_ref[...], grads, TN)
    for (dq, dh), send in zip(moves, sends, strict=True):
        target = (lax.rem(q + dq, groups) * 2 + lax.rem(h + dh, 2)) * 2 + c
        send[0:rows] = total_ref[aligned(target, rows, 8), :].astype(send.dtype)
    sends[1][rows:, 0 : 2 * width] = pack(give_ref[...])


def expert_body(moves, groups, width, *refs):
    count = len(moves)
    blocks = refs[: 2 * count]
    own_ref, other_ref, full_ref, hid_ref, stage_ref = refs[2 * count :]
    q, h, c = lax.axis_index("q"), lax.axis_index("h"), lax.axis_index("c")
    slots = own_ref.shape[0]
    rows = blocks[0].shape[0] - slots // 2
    for i, (dq, dh) in enumerate(moves):
        source = (lax.rem(q + (groups - dq), groups) * 2 + lax.rem(h + dh, 2)) * 2
        for side, core in ((0, c), (count, 1 - c)):
            stage_ref[aligned(source + core, rows, 8), :] = blocks[side + i][0:rows].astype(stage_ref.dtype)
    for i in range(2):
        hid_ref[i * slots : (i + 1) * slots] = unpack(blocks[i][rows:], width)
    full = stage_ref[...].astype(BF16)
    out = dot(hid_ref[...], full, NN).astype(BF16)
    own_ref[...] = out[0:slots]
    other_ref[...] = out[slots:]
    full_ref[...] = full


def hidden_grad_body(grad_ref, full_ref, keep_ref, give_ref):
    h = lax.axis_index("h")
    slots = keep_ref.shape[0]
    full = full_ref[...]
    keep_ref[...] = dot(grad_ref[aligned(h, slots, 16), :], full, NT)
    give_ref[...] = dot(grad_ref[aligned(1 - h, slots, 16), :], full, NT).astype(BF16)


def combine_body(table_ref, index_ref, cot_ref, *refs):
    pieces, (layer_ref, route_ref, arrived_ref) = refs[:-3], refs[-3:]
    count = len(pieces)
    unit = pieces[0].shape[0] // 2
    slots, half = count * unit, arrived_ref.shape[1]
    s = lax.axis_index("ep")
    for step, piece in enumerate(pieces):
        source = origin(s, step, count)
        for g in range(2):
            arrived_ref[aligned(g * count + source, unit, 16), :] = piece[g * unit : (g + 1) * unit]
    scores = None
    for g in range(2):
        rows = arrived_ref[g * slots : (g + 1) * slots]
        mixed = dot(table_ref[...], jnp.concatenate([rows] * 3, axis=0), TN)
        layer_ref[:, g * half : (g + 1) * half] = mixed.astype(BF16)
        part = dot(rows, cot_ref[:, g * half : (g + 1) * half], NT)
        scores = part if scores is None else scores + part
    position = lax.broadcasted_iota(jnp.int32, scores.shape, 0).astype(F32)
    for k in range(index_ref.shape[0]):
        hit = position == index_ref[k : k + 1]
        route_ref[k : k + 1] = jnp.sum(jnp.where(hit, scores, 0.0), axis=0, keepdims=True)


def finish_body(moves, keep_ref, *refs):
    count = len(moves)
    terms, (hidden_ref, weight_ref) = refs[:count], refs[count:]
    h = lax.axis_index("h")
    rows, half = terms[0].shape
    given = unpack(terms[1][rows:], hidden_ref.shape[1])
    hidden_ref[...] = (keep_ref[...] + given.astype(F32)).astype(BF16)
    for side in range(2):
        total = None
        for (_, dh), term in zip(moves, terms, strict=True):
            if dh == side:
                value = term[0:rows].astype(F32)
                total = value if total is None else total + value
        weight_ref[:, aligned(h if side == 0 else 1 - h, half, 128)] = total


def local(route_ids, route_weights, hidden, down_weight, cotangent):
    groups = lax.axis_size("q")
    experts = lax.axis_size("ep")
    tokens, features = cotangent.shape
    capacity, width = hidden.shape[3], hidden.shape[4]
    rows = down_weight.shape[1]
    slots = experts * capacity
    choices = route_ids.shape[1]
    half = features // 2
    moves = [(0, 0), (0, 1)] + [(dq, dh) for dq in range(1, groups) for dh in range(2)]
    swap = [(0, 1), (1, 0)]

    def move(x, step):
        dq, dh = step
        pairs = [(a * 2 + b, (a + dq) % groups * 2 + (b + dh) % 2) for a in range(groups) for b in range(2)]
        return lax.ppermute(x, ("q", "h"), pairs)

    def swap_core(x):
        return lax.ppermute(x, "c", swap)

    def exchange(x):
        parts = x.reshape(2 * experts, capacity, half)
        return lax.all_to_all(parts, ("h", "ep"), split_axis=0, concat_axis=0, tiled=True).reshape(x.shape)

    plain = sds((rows, half), BF16)
    joined = sds((rows + slots // 2, half), BF16)
    parts = sds((2 * slots, half), BF16)
    part = sds((slots, half), BF16)
    same, cross, same_hid, cross_hid, ids, weights, cot = call(
        load_body,
        (plain, plain, joined, joined, sds((choices, tokens), route_ids.dtype), sds((choices, tokens), F32), sds(cotangent.shape, BF16)),
        [pltpu.VMEM((slots, width), BF16), pltpu.SemaphoreType.DMA((8,))],
        fetched=True,
    )(down_weight[0], route_ids.T, route_weights.T, cotangent, hidden.reshape(slots, width))

    blocks = [same_hid, move(cross_hid, moves[1])]
    blocks += [move(cross if step[1] else same, step) for i, step in enumerate(moves) if i > 1]
    blocks += [swap_core(b) for b in blocks]
    sent = call(
        functools.partial(route_body, experts, capacity), parts, flops=2 * slots * tokens * features
    )(ids, weights, cot)
    table, index = call(
        functools.partial(tables_body, experts, capacity),
        (sds((3 * slots, tokens), BF16), sds((choices, tokens), F32)),
        flops=2 * tokens * tokens * experts,
    )(ids, weights)
    grads = exchange(sent)
    partner_grads = swap_core(grads)

    own_out, other_out, full = call(
        functools.partial(expert_body, moves, groups, width),
        (part, part, sds((width, half), BF16)),
        [
            pltpu.VMEM((2 * slots, width), BF16),
            pltpu.VMEM((width, half), BF16 if rows % 16 == 0 else F32),
        ],
        flops=8 * slots * width * half,
    )(*blocks)
    other_half = lax.ppermute(other_out, "h", swap)

    keep, give = call(
        hidden_grad_body, (sds((slots, width), F32), sds((slots, width), BF16)), flops=4 * slots * width * half
    )(grads, full)

    weight_terms = call(
        functools.partial(weight_grad_body, moves, groups, width),
        (sds((rows, half), F32), joined, *[plain] * (len(moves) - 2)),
        [pltpu.VMEM((4 * slots, width), BF16), pltpu.VMEM((width, half), F32)],
        flops=8 * slots * width * half,
    )(blocks[0], blocks[1], blocks[len(moves)], blocks[len(moves) + 1], grads, partner_grads, give)
    terms = [weight_terms[0]] + [move(weight_terms[i], step) for i, step in enumerate(moves) if i]

    parcels = call(join_body, (sds((2 * capacity, half), BF16),) * experts, flops=slots)(own_out, other_half)
    arrived = [parcels[0]]
    for step in range(1, experts):
        pairs = [(e, int(peer(e, step, experts))) for e in range(experts)]
        arrived.append(lax.ppermute(parcels[step], "ep", pairs))

    layer_out, route_grad = call(
        combine_body,
        (sds((tokens, features), BF16), sds((choices, tokens), F32)),
        [pltpu.VMEM((2 * slots, half), BF16)],
        flops=8 * slots * tokens * features,
    )(table, index, cot, *arrived)

    hidden_grad, weight_grad = call(
        functools.partial(finish_body, moves),
        (sds((slots, width), BF16), sds((rows, features), F32)),
        flops=rows * features,
    )(keep, *terms)
    return layer_out, route_grad.T, hidden_grad.reshape(hidden.shape), weight_grad[None]


def solution(mesh):
    edp, ep = mesh.shape["edp"], mesh.shape["ep"]
    fine = Mesh(mesh.devices.reshape(edp // 4, 2, 2, ep), ("q", "h", "c", "ep"))
    group = ("q", "h", "c")
    tokens = P(group + ("ep",), None)
    slots = P(group, "ep", None, None, None)
    weights = P("ep", group, None)
    return jax.shard_map(
        local,
        mesh=fine,
        in_specs=(tokens, tokens, slots, weights, tokens),
        out_specs=(tokens, tokens, slots, weights),
        check_vma=False,
    )
```
